32 devices in a mesh: row: 4 (over x, core), col: 8 (over z, y).
Axes of the slice: x: 2, y: 2, z: 4, core: 2. Of those that a mesh axis runs over, the one named last changes fastest.
Arguments:
- tokens: bfloat16 [1024, 4096], P('col', 'row'), may hold values from -12 to 12
- target: bfloat16 [1024, 4096], P('col', 'row'), may hold values from -6 to 6
- gate_weight: bfloat16 [4096, 5504], P('row', 'col'), may hold values from -0.09375 to 0.09375
- up_weight: bfloat16 [4096, 5504], P('row', 'col'), may hold values from -0.09375 to 0.09375
- down_weight: bfloat16 [5504, 4096], P('col', 'row'), may hold values from -0.078125 to 0.078125
- probe_gate: int32 [4096, 5504], P('row', 'col'), may hold values from 0 to 1
- probe_up: int32 [4096, 5504], P('row', 'col'), may hold values from 0 to 1
- probe_down: int32 [5504, 4096], P('col', 'row'), may hold values from 0 to 1
- first_gate: float32 [4096, 5504], P('row', 'col'), may hold values from -1.8 to 1.8
- first_up: float32 [4096, 5504], P('row', 'col'), may hold values from -1.8 to 1.8
- first_down: float32 [5504, 4096], P('col', 'row'), may hold values from -1.8 to 1.8
- second_gate: float32 [4096, 5504], P('row', 'col'), may hold values from 0.01 to 0.2
- second_up: float32 [4096, 5504], P('row', 'col'), may hold values from 0.01 to 0.2
- second_down: float32 [5504, 4096], P('col', 'row'), may hold values from 0.01 to 0.2
Outputs:
- new_first_gate: float32 [4096, 5504], P('row', 'col')
- new_first_up: float32 [4096, 5504], P('row', 'col')
- new_first_down: float32 [5504, 4096], P('col', 'row')
- new_second_gate: float32 [4096, 5504], P('row', 'col')
- new_second_up: float32 [4096, 5504], P('row', 'col')
- new_second_down: float32 [5504, 4096], P('col', 'row')
- update_gate: float32 [4096, 5504], P('row', 'col')
- update_up: float32 [4096, 5504], P('row', 'col')
- update_down: float32 [5504, 4096], P('col', 'row')
The draws below stay inside these ranges and needn't reach their ends.
Inputs may be any that keep to these rules, and one draw needn't show every extreme that they name: `probe_gate`: probe bits; the probe is 2 p - 1. `probe_up`: probe bits; the probe is 2 p - 1. `probe_down`: probe bits; the probe is 2 p - 1.
All inputs are finite; a program needn't handle non-finite values.
Results may differ from the reference program's by a relative error of at most 0.038.
Values may be sent and summed in bfloat16 or wider, within the bound.
No kernel may reach another device: no remote copies, remote signals or barrier semaphores. Data moves between devices by JAX's collectives and lax.ppermute only.
A program may use at most 256 MiB of HBM per device.

```python
import math
import jax
import jax.numpy as jnp
from jax import lax

D = 4096
FF = 5504
STEP = 10
TOKENS = 1024
N_ROW = 4
N_COL = 8


def draw_tokens(key, part):
    first_key, second_key = jax.random.split(jax.random.fold_in(key, 17), 2)
    position = jnp.arange(D, dtype=jnp.float32) / D
    scales = 0.1 * 10.0 ** (0.5 * position + 0.5 * jax.random.uniform(first_key, (D,), jnp.float32))
    rows = jnp.arange(TOKENS, dtype=jnp.float32) / TOKENS
    rising = 3.0 ** rows
    base = jnp.clip(jax.random.normal(second_key, (TOKENS, D), jnp.float32), -4.0, 4.0)
    return (base * scales[None, :] * rising[:, None]).astype(jnp.bfloat16)


def plant(entries, rng, least, largest):
    dims = entries.shape
    spot = [jax.random.randint(jax.random.fold_in(rng, axis), (), 0, dims[axis]) for axis in range(len(dims))]
    entries = entries.at[tuple(spot)].set(least)
    longest = dims.index(max(dims))
    spot[longest] = (spot[longest] + 1) % dims[longest]
    return entries.at[tuple(spot)].set(largest)


def levels(own_key, extent, shards, least, high):
    gain = 1.0
    for axis_at, blocks in shards:
        steps = jax.random.uniform(jax.random.fold_in(jax.random.fold_in(own_key, 6), axis_at), (blocks,), jnp.float32, least / len(shards), high / len(shards))
        gain = gain * jnp.repeat(jnp.exp(steps), extent[axis_at] // blocks).reshape((-1,) + (1,) * (len(extent) - 1 - axis_at))
    return gain


def centred(own_key, extent, spread, reach, cuts=(), kind=jnp.bfloat16):
    array = jax.random.normal(own_key, extent, jnp.float32) * spread
    if len(cuts) > 0:
        array = levels(own_key, extent, cuts, -0.22, 0.18) * array
    return jnp.clip(array, min=-reach, max=reach).astype(kind)


def setup_inputs(seed: int = 0) -> dict:
    key_of = jax.random.split(jax.random.key(seed), 15)
    tokens = draw_tokens(jax.random.fold_in(key_of[14], 71), 0)
    target = centred(key_of[1], (TOKENS, D), 1.0, 6.0, ((0, 8), (1, 4)))
    gate_weight = centred(key_of[2], (D, FF), D ** -0.5, 0.09375, ((0, 4), (1, 8)))
    up_weight = centred(key_of[3], (D, FF), D ** -0.5, 0.09375, ((0, 4), (1, 8)))
    down_weight = centred(key_of[4], (FF, D), FF ** -0.5, 0.078125, ((0, 8), (1, 4)))
    probe_gate = plant(jax.random.randint(key_of[5], (D, FF), 0, 2), jax.random.fold_in(key_of[5], 1), 0, 1).astype(jnp.int32)
    probe_up = plant(jax.random.randint(key_of[6], (D, FF), 0, 2), jax.random.fold_in(key_of[6], 1), 0, 1).astype(jnp.int32)
    probe_down = plant(jax.random.randint(key_of[7], (FF, D), 0, 2), jax.random.fold_in(key_of[7], 1), 0, 1).astype(jnp.int32)
    first_gate = centred(key_of[8], (D, FF), 0.3, 1.8, ((0, 4), (1, 8)), jnp.float32)
    first_up = centred(key_of[9], (D, FF), 0.3, 1.8, ((0, 4), (1, 8)), jnp.float32)
    first_down = centred(key_of[10], (FF, D), 0.3, 1.8, ((0, 8), (1, 4)), jnp.float32)
    second_gate = jnp.clip(jnp.exp(math.log(0.2) - 2.9957323 * jax.random.uniform(key_of[11], (D, FF), jnp.float32) ** levels(key_of[11], (D, FF), ((0, 4), (1, 8)), -0.2, 0.2)), 0.01, 0.2)
    second_up = jnp.clip(jnp.exp(math.log(0.2) - 2.9957323 * jax.random.uniform(key_of[12], (D, FF), jnp.float32) ** levels(key_of[12], (D, FF), ((0, 4), (1, 8)), -0.2, 0.2)), 0.01, 0.2)
    second_down = jnp.clip(jnp.exp(math.log(0.2) - 2.9957323 * jax.random.uniform(key_of[13], (FF, D), jnp.float32) ** levels(key_of[13], (FF, D), ((0, 8), (1, 4)), -0.2, 0.2)), 0.01, 0.2)
    return {"tokens": tokens, "target": target, "gate_weight": gate_weight, "up_weight": up_weight, "down_weight": down_weight, "probe_gate": probe_gate, "probe_up": probe_up, "probe_down": probe_down, "first_gate": first_gate, "first_up": first_up, "first_down": first_down, "second_gate": second_gate, "second_up": second_up, "second_down": second_down}


def activation(pre):
    sig = jax.nn.sigmoid(pre)
    act = pre * sig
    slope = sig * (1.0 + pre * (1.0 - sig))
    bend = sig * (1.0 - sig) * (2.0 + pre * (1.0 - 2.0 * sig))
    return (act, slope, bend)

def block_mean(values):
    height, breadth = values.shape
    means = values.reshape(height // 4, 4, breadth // 4, 4).mean(axis=(1, 3))
    return jnp.broadcast_to(means[:, None, :, None], (height // 4, 4, breadth // 4, 4)).reshape(height, breadth)

def matmul(left, right):
    return jnp.dot(left, right, preferred_element_type=jnp.float32)

def rounded_runs(term_of, pieces):
    total = None
    for index in range(pieces):
        part = term_of(index)
        part = jax.tree.map(lambda value: lax.optimization_barrier(value.astype(jnp.bfloat16)).astype(jnp.float32), part)
        total = part if total is None else jax.tree.map(lambda first, second: first + second, total, part)
    return total

def reference(tokens, target, gate_weight, up_weight, down_weight, probe_gate, probe_up, probe_down, first_gate, first_up, first_down, second_gate, second_up, second_down):
    sign_gate = (2 * probe_gate - 1).astype(jnp.bfloat16)
    sign_up = (2 * probe_up - 1).astype(jnp.bfloat16)
    sign_down = (2 * probe_down - 1).astype(jnp.bfloat16)
    feat_run = D // N_ROW
    unit_run = FF // N_COL

    def project(index):
        lower = index * feat_run
        block = tokens[:, lower:lower + feat_run]
        return (matmul(block, gate_weight[lower:lower + feat_run]), matmul(block, up_weight[lower:lower + feat_run]), matmul(block, sign_gate[lower:lower + feat_run]), matmul(block, sign_up[lower:lower + feat_run]))
    pre_gate, pre_up, dot_gate, dot_up = rounded_runs(project, N_ROW)
    act, slope, bend = activation(pre_gate)
    hidden = (act * pre_up).astype(jnp.bfloat16)
    hidden_dot = (slope * dot_gate * pre_up + act * dot_up).astype(jnp.bfloat16)

    def forward(index):
        lower = index * unit_run
        plain = hidden[:, lower:lower + unit_run]
        tangent = hidden_dot[:, lower:lower + unit_run]
        weight = down_weight[lower:lower + unit_run]
        return (matmul(plain, weight), matmul(tangent, weight) + matmul(plain, sign_down[lower:lower + unit_run]))
    out_val, out_dot = rounded_runs(forward, N_COL)
    err = (out_val - target.astype(jnp.float32)).astype(jnp.bfloat16)
    err_dot = out_dot.astype(jnp.bfloat16)

    def backward(index):
        lower = index * feat_run
        err_part = err[:, lower:lower + feat_run]
        dot_part = err_dot[:, lower:lower + feat_run]
        weight = down_weight[:, lower:lower + feat_run]
        return (matmul(err_part, weight.T), matmul(dot_part, weight.T) + matmul(err_part, sign_down[:, lower:lower + feat_run].T))
    d_hidden, d_hidden_dot = rounded_runs(backward, N_ROW)
    grad_down = matmul(hidden.T, err)
    hess_down = matmul(hidden_dot.T, err) + matmul(hidden.T, err_dot)
    d_gate = (d_hidden * pre_up * slope).astype(jnp.bfloat16)
    d_up = (d_hidden * act).astype(jnp.bfloat16)
    dd_gate = (d_hidden_dot * pre_up * slope + d_hidden * dot_up * slope + d_hidden * pre_up * bend * dot_gate).astype(jnp.bfloat16)
    dd_up = (d_hidden_dot * act + d_hidden * slope * dot_gate).astype(jnp.bfloat16)
    grad_gate = matmul(tokens.T, d_gate)
    grad_up = matmul(tokens.T, d_up)
    hess_gate = matmul(tokens.T, dd_gate)
    hess_up = matmul(tokens.T, dd_up)
    curv_gate = block_mean(jnp.abs(sign_gate.astype(jnp.float32) * hess_gate))
    curv_up = block_mean(jnp.abs(sign_up.astype(jnp.float32) * hess_up))
    curv_down = block_mean(jnp.abs(sign_down.astype(jnp.float32) * hess_down))
    count = 3.0 * D * FF
    total_grad = jnp.sum(grad_gate * grad_gate) + jnp.sum(grad_up * grad_up) + jnp.sum(grad_down * grad_down)
    total_curv = jnp.sum(curv_gate * curv_gate) + jnp.sum(curv_up * curv_up) + jnp.sum(curv_down * curv_down)
    rms_grad = jnp.sqrt(total_grad / count + 1e-06)
    rms_curv = jnp.sqrt(total_curv / count + 1e-06)
    fix_first = 1.0 - 0.9 ** STEP
    fix_second = 1.0 - 0.95 ** STEP
    firsts = []
    seconds = []
    updates = []
    for grad, curv, first, second in ((grad_gate, curv_gate, first_gate, second_gate), (grad_up, curv_up, first_up, second_up), (grad_down, curv_down, first_down, second_down)):
        new_first = 0.9 * first + 0.1 * (grad / rms_grad)
        scaled = curv / rms_curv
        new_second = 0.95 * second + 0.05 * (scaled * scaled)
        firsts.append(new_first)
        seconds.append(new_second)
        updates.append(new_first / fix_first / (jnp.sqrt(new_second / fix_second) + 1e-08))
    return (firsts[0], firsts[1], firsts[2], seconds[0], seconds[1], seconds[2], updates[0], updates[1], updates[2])
```

```python
import jax
import jax.numpy as jnp
from jax import lax
from jax.experimental import pallas as pl
from jax.experimental.pallas import tpu as pltpu
from jax.sharding import PartitionSpec as P


STEP = 10
BF = jnp.bfloat16
F32 = jnp.float32


def dot(left, right, inner):
    return lax.dot_general(left, right, (((inner[0],), (inner[1],)), ((), ())), preferred_element_type=F32)


def pick(blocks, index):
    chosen = blocks[0]
    for at in range(1, len(blocks)):
        chosen = jnp.where(index == at, blocks[at], chosen)
    return chosen


def pair_swap(value, axis, size):
    return lax.ppermute(value, axis, [(i, i ^ 1) for i in range(size)])


def ring_up(value, axis, size):
    return lax.ppermute(value, axis, [(i, (i + 2) % size) for i in range(size)])


def total_over_all(value, sizes):
    for axis, size in sizes:
        step = 1
        while step < size:
            if size % (2 * step) == 0:
                value = value + lax.ppermute(value, axis, [(i, i ^ step) for i in range(size)])
                step *= 2
            else:
                raise ValueError("axis size")
    return value


def sign_kernel(gate_ref, up_ref, down_ref, sign_gate_ref, sign_up_ref, sign_down_ref):
    for probe, sign in ((gate_ref, sign_gate_ref), (up_ref, sign_up_ref), (down_ref, sign_down_ref)):
        sign[...] = (2 * probe[...] - 1).astype(F32).astype(BF)


def side(feats):
    return 256 if feats % 256 == 0 else 128


def cols_tile(rows, tile):
    return pl.BlockSpec((rows, tile), lambda i: (0, i))


def fixed(shape):
    return pl.BlockSpec(shape, lambda i: (0, 0))


def signs(*probes):
    width, feats = probes[0].shape
    tile = side(feats)
    specs = [cols_tile(width, tile)] * 3
    return pl.pallas_call(
        sign_kernel,
        grid=(feats // tile,),
        in_specs=specs,
        out_specs=specs,
        out_shape=[jax.ShapeDtypeStruct(p.shape, BF) for p in probes],
        name="signs",
    )(*probes)


def same_block():
    down = lax.broadcasted_iota(jnp.int32, (256, 256), 0) >> 2
    across = lax.broadcasted_iota(jnp.int32, (256, 256), 1) >> 2
    return jnp.where(down == across, 1.0, 0.0).astype(BF)


def finish_weight(grad, hess, sign, grad_ref, curv_ref, grad_sum, curv_sum):
    height, breadth = hess.shape
    grad_ref[...] = grad
    grad_sum[...] += jnp.sum(grad * grad, axis=0, keepdims=True)
    same = same_block()
    size = jnp.abs(sign.astype(F32) * hess).astype(BF)
    total = curv_sum[...]
    for top in range(0, height, 256):
        tall = min(256, height - top)
        sums = jnp.dot(same[:tall, :tall], size[top : top + tall], preferred_element_type=F32)
        means = jnp.dot(
            (sums * 0.0625).astype(BF), same[:breadth, :breadth], preferred_element_type=F32
        )
        curv_ref[top : top + tall, :] = means
        total = total + jnp.sum(means * means, axis=0, keepdims=True)
    curv_sum[...] = total


def pack_sums(grad_sum, curv_sum):
    lane = lax.broadcasted_iota(jnp.int32, (8, 128), 1)
    first = jnp.where(lane == 0, jnp.sum(grad_sum[...]), 0.0)
    return jnp.where(lane == 1, jnp.sum(curv_sum[...]), first)


def in_order(core, refs):
    shards = []
    for current, other in zip(refs[::2], refs[1::2]):
        one = current[...]
        two = other[...]
        shards += [jnp.where(core == 0, one, two), jnp.where(core == 0, two, one)]
    return jnp.concatenate(shards, axis=0)


def down_kernel(pieces, *refs):
    core_ref, panel_ref, sign_ref = refs[:3]
    err_refs = refs[3 : 3 + pieces]
    dot_refs = refs[3 + pieces : 3 + 2 * pieces]
    grad_ref, curv_ref, pack_ref, grad_sum, curv_sum = refs[3 + 2 * pieces :]

    @pl.when(pl.program_id(0) == 0)
    def _():
        grad_sum[...] = jnp.zeros_like(grad_sum)
        curv_sum[...] = jnp.zeros_like(curv_sum)

    width = sign_ref.shape[0]
    err = in_order(core_ref[0], err_refs)
    err_dot = in_order(core_ref[0], dot_refs)
    plain = panel_ref[:width, :]
    grad = jnp.dot(plain, err, preferred_element_type=F32)
    hess = jnp.dot(panel_ref[width:, :], err, preferred_element_type=F32)
    hess = hess + jnp.dot(plain, err_dot, preferred_element_type=F32)
    finish_weight(grad, hess, sign_ref[...], grad_ref, curv_ref, grad_sum, curv_sum)

    @pl.when(pl.program_id(0) == pl.num_programs(0) - 1)
    def _():
        pack_ref[...] = pack_sums(grad_sum, curv_sum)


def down_grads(core, panel, sign, errs, dots):
    width, feats = sign.shape
    tile = side(feats)
    each = [cols_tile(errs[0].shape[0], tile)] * len(errs)
    return pl.pallas_call(
        lambda *refs: down_kernel(len(errs), *refs),
        grid=(feats // tile,),
        in_specs=[
            pl.BlockSpec(memory_space=pltpu.SMEM), fixed(panel.shape), cols_tile(width, tile), *each, *each
        ],
        out_specs=[cols_tile(width, tile), cols_tile(width, tile), fixed((8, 128))],
        out_shape=[
            jax.ShapeDtypeStruct((width, feats), F32),
            jax.ShapeDtypeStruct((width, feats), F32),
            jax.ShapeDtypeStruct((8, 128), F32),
        ],
        scratch_shapes=[pltpu.VMEM((1, tile), F32), pltpu.VMEM((1, tile), F32)],
        compiler_params=pltpu.CompilerParams(dimension_semantics=("arbitrary",)),
        cost_estimate=pl.CostEstimate(
            flops=6 * width * feats * panel.shape[1], transcendentals=0, bytes_accessed=12 * width * feats
        ),
        name="down_grads",
    )(core, panel, sign, *errs, *dots)


def wide_kernel(pieces, *refs):
    core_ref, sign_gate_ref, sign_up_ref, before_ref, cot_ref = refs[:5]
    token_refs = refs[5 : 5 + pieces]
    grad_gate_ref, curv_gate_ref, grad_up_ref, curv_up_ref, pack_ref, grad_sum, curv_sum = refs[5 + pieces :]

    @pl.when(pl.program_id(0) == 0)
    def _():
        grad_sum[...] = jnp.zeros_like(grad_sum)
        curv_sum[...] = jnp.zeros_like(curv_sum)

    width = sign_gate_ref.shape[0]
    tokens = in_order(core_ref[0], token_refs)

    def product(at):
        return jnp.dot(cot_ref[at * width : (at + 1) * width, :], tokens, preferred_element_type=F32)

    finish_weight(
        product(0), product(2), sign_gate_ref[...], grad_gate_ref, curv_gate_ref, grad_sum, curv_sum
    )
    finish_weight(product(1), product(3), sign_up_ref[...], grad_up_ref, curv_up_ref, grad_sum, curv_sum)

    @pl.when(pl.program_id(0) == pl.num_programs(0) - 1)
    def _():
        pack_ref[...] = before_ref[...] + pack_sums(grad_sum, curv_sum)


def wide_grads(core, sign_gate, sign_up, before, cots, tokens):
    width, feats = sign_gate.shape
    tile = side(feats)
    out = cols_tile(width, tile)
    count = cots.shape[1]
    return pl.pallas_call(
        lambda *refs: wide_kernel(len(tokens), *refs),
        grid=(feats // tile,),
        in_specs=[
            pl.BlockSpec(memory_space=pltpu.SMEM), out, out, fixed((8, 128)), fixed(cots.shape),
            *[cols_tile(t.shape[0], tile) for t in tokens],
        ],
        out_specs=[out, out, out, out, fixed((8, 128))],
        out_shape=[jax.ShapeDtypeStruct((width, feats), F32)] * 4 + [jax.ShapeDtypeStruct((8, 128), F32)],
        scratch_shapes=[pltpu.VMEM((1, tile), F32), pltpu.VMEM((1, tile), F32)],
        compiler_params=pltpu.CompilerParams(dimension_semantics=("arbitrary",)),
        cost_estimate=pl.CostEstimate(
            flops=8 * width * feats * count, transcendentals=0, bytes_accessed=20 * width * feats
        ),
        name="wide_grads",
    )(core, sign_gate, sign_up, before, cots, *tokens)


def cotangent_kernel(keep_ref, send_ref, by_keep_ref, by_send_ref, *refs):
    out_ref = refs[-1]
    width = keep_ref.shape[0] // 2
    count = keep_ref.shape[1]
    for at, (d_ref, by_ref) in enumerate(((keep_ref, by_keep_ref), (send_ref, by_send_ref))):
        lanes = slice(at * count, (at + 1) * count)
        d_hidden = d_ref[:width].astype(F32)
        d_hidden_dot = d_ref[width:].astype(F32)
        for_gate = by_ref[:width].astype(F32)
        for_up = by_ref[width : 2 * width].astype(F32)
        out_ref[:width, lanes] = (d_hidden * for_gate).astype(BF)
        out_ref[width : 2 * width, lanes] = (d_hidden * for_up).astype(BF)
        out_ref[2 * width : 3 * width, lanes] = (
            d_hidden_dot * for_gate + d_hidden * by_ref[2 * width : 3 * width].astype(F32)
        ).astype(BF)
        out_ref[3 * width :, lanes] = (
            d_hidden_dot * for_up + d_hidden * by_ref[3 * width :].astype(F32)
        ).astype(BF)


def cotangents_of(at, pieces, panel, *args):
    height = args[2].shape[0]
    wide = 2 * args[0].shape[1]
    more = [] if panel is None else [panel]
    return pl.pallas_call(
        cotangent_kernel,
        grid=(1,),
        in_specs=[fixed(v.shape) for v in args] + [pl.BlockSpec(memory_space=pl.ANY)] * len(more),
        out_specs=pl.BlockSpec((height, wide), lambda i: (0, at)),
        out_shape=jax.ShapeDtypeStruct((height, wide * pieces), BF),
        input_output_aliases={4: 0} if more else {},
        cost_estimate=pl.CostEstimate(
            flops=4 * height * wide, transcendentals=0, bytes_accessed=6 * height * wide
        ),
        name="cotangents",
    )(*args, *more)


def update_kernel(scale_ref, *refs):
    fix_first = 1.0 - 0.9**STEP
    fix_second = 1.0 - 0.95**STEP
    by_grad = scale_ref[0]
    by_curv = scale_ref[1]
    for at in range(3):
        grad, curv, first, second = (refs[4 * at + n][...] for n in range(4))
        first_ref, second_ref, update_ref = (refs[12 + 3 * n + at] for n in range(3))
        new_first = 0.9 * first + 0.1 * (grad * by_grad)
        scaled = curv * by_curv
        new_second = 0.95 * second + 0.05 * (scaled * scaled)
        first_ref[...] = new_first
        second_ref[...] = new_second
        update_ref[...] = new_first * (1.0 / fix_first) / (jnp.sqrt(new_second * (1.0 / fix_second)) + 1e-08)


def update(scales, weights):
    width, feats = weights[0][0].shape
    tall = cols_tile(width, 128)
    shapes = [jax.ShapeDtypeStruct(w[0].shape, F32) for w in weights]
    return pl.pallas_call(
        update_kernel,
        grid=(feats // 128,),
        in_specs=[pl.BlockSpec(memory_space=pltpu.SMEM)] + [tall] * 12,
        out_specs=[tall] * 9,
        out_shape=shapes * 3,
        name="update",
    )(scales, *weights[0], *weights[1], *weights[2])


def activation(pre):
    sig = jax.nn.sigmoid(pre)
    act = pre * sig
    slope = sig * (1.0 + pre * (1.0 - sig))
    bend = sig * (1.0 - sig) * (2.0 + pre * (1.0 - 2.0 * sig))
    return (act, slope, bend)


def make_body(n_row, n_col):
    outer = n_row // 2
    rings = n_col // 2
    groups = rings // outer
    if n_row % 2 or n_col % 2 or rings % outer:
        raise ValueError("mesh")

    def body(
        tokens, target, gate_weight, up_weight, down_weight, probe_gate, probe_up, probe_down,
        first_gate, first_up, first_down, second_gate, second_up, second_down,
    ):
        row = lax.axis_index("row")
        core = row % 2
        chip = row // 2
        core_line = jnp.reshape(core, (1,)).astype(jnp.int32)
        gate_weight, up_weight, probe_gate, probe_up, first_gate, first_up, second_gate, second_up = (
            v.T
            for v in (
                gate_weight, up_weight, probe_gate, probe_up, first_gate, first_up, second_gate, second_up
            )
        )
        width, feats = gate_weight.shape
        count = tokens.shape[0]
        sign_gate, sign_up, sign_down = signs(probe_gate, probe_up, probe_down)

        token_pieces = []
        pre_keeps = []
        current = tokens
        for k in range(rings):
            other = pair_swap(current, "col", n_col)
            following = ring_up(current, "col", n_col) if k < rings - 1 else None
            keep = jnp.where(core == 0, current, other)
            send = jnp.where(core == 0, other, current)
            piece = jnp.concatenate([keep, send], axis=0)
            token_pieces += [current, other]
            current = following
            parts = [dot(matrix, piece, (1, 1)) for matrix in (gate_weight, up_weight, sign_gate, sign_up)]
            sent = jnp.concatenate([part[:, count:].astype(BF) for part in parts], axis=0)
            kept = jnp.concatenate([part[:, :count] for part in parts], axis=0)
            pre_keeps.append(kept + pair_swap(sent, "row", n_row).astype(F32))

        hidden_keeps = []
        hidden_sends = []
        owned = []
        for g in range(groups):
            mine = pre_keeps[g * outer : (g + 1) * outer]
            current = pick(mine, (chip - 1) % outer)
            for s in range(1, outer):
                got = ring_up(current.astype(BF), "row", n_row)
                current = got.astype(F32) + pick(mine, (chip - s - 1) % outer)
            pre_gate = current[:width]
            pre_up = current[width : 2 * width]
            dot_gate = current[2 * width : 3 * width]
            dot_up = current[3 * width :]
            act, slope, bend = activation(pre_gate)
            owned.append(
                jnp.concatenate(
                    [
                        (pre_up * slope).astype(BF),
                        act.astype(BF),
                        (dot_up * slope + pre_up * bend * dot_gate).astype(BF),
                        (slope * dot_gate).astype(BF),
                    ],
                    axis=0,
                )
            )
            hidden = (act * pre_up).astype(BF)
            hidden_dot = (slope * dot_gate * pre_up + act * dot_up).astype(BF)
            keeps = by_owner(gather_blocks(jnp.concatenate([hidden, hidden_dot], axis=0)), chip)
            both = jnp.concatenate(keeps, axis=1)
            sends = pair_swap(both, "row", n_row)
            hidden_keeps.append(both)
            hidden_sends.append(sends)

        near = ([], [])
        far = ([], [])
        for g in range(groups):
            sides = []
            for panel in (hidden_keeps[g], hidden_sends[g]):
                value = dot(panel[:width], down_weight, (0, 0))
                along = dot(panel[width:], down_weight, (0, 0)) + dot(panel[:width], sign_down, (0, 0))
                sides.append((value, along))
            for j in range(outer):
                for part in range(2):
                    own = sides[0][part][j * count : (j + 1) * count]
                    alien = sides[1][part][j * count : (j + 1) * count]
                    near[part].append(jnp.where(core == 0, own, alien))
                    far[part].append(jnp.where(core == 0, alien, own).astype(BF))
        order = [*range(1, rings), 0]
        reduced = {}
        for k in order:
            for part in range(2):
                reduced[k, part] = near[part][k] + pair_swap(far[part][k], "col", n_col).astype(F32)
        outputs = [reduced[order[0], part] for part in range(2)]
        for k in order[1:]:
            for part in range(2):
                moved = ring_up(outputs[part].astype(BF), "col", n_col)
                outputs[part] = moved.astype(F32) + reduced[k, part]
        errors = [(outputs[0] - target.astype(F32)).astype(BF), outputs[1].astype(BF)]

        pre_parts = []
        for g in range(groups):
            got = gather_blocks(owned[g])
            errors[0], *got = lax.optimization_barrier((errors[0], *got))
            keeps = by_owner(got, chip)
            for j in range(outer):
                pre_parts.append((keeps[j], pair_swap(keeps[j], "row", n_row)))

        error_pieces = ([], [])
        error_shards = ([], [])
        cots = None
        for k in range(rings):
            for part in range(2):
                current = errors[part]
                other = pair_swap(current, "col", n_col)
                if k < rings - 1:
                    errors[part] = ring_up(current, "col", n_col)
                keep = jnp.where(core == 0, current, other)
                send = jnp.where(core == 0, other, current)
                error_shards[part].extend([current, other])
                error_pieces[part].append(jnp.concatenate([keep, send], axis=0))
            err, err_dot = error_pieces[0][k], error_pieces[1][k]
            plain = dot(down_weight, err, (1, 1))
            along = dot(down_weight, err_dot, (1, 1)) + dot(sign_down, err, (1, 1))
            sent = jnp.concatenate([plain[:, count:].astype(BF), along[:, count:].astype(BF)], axis=0)
            kept = jnp.concatenate([plain[:, :count], along[:, :count]], axis=0)
            total = kept + pair_swap(sent, "row", n_row).astype(F32)
            moving = total.astype(BF)
            for _ in range(1, outer):
                moving = ring_up(moving, "row", n_row)
                total = total + moving.astype(F32)
            keep_d = total.astype(BF)
            send_d = pair_swap(keep_d, "row", n_row)
            cots = cotangents_of(k, rings, cots, keep_d, send_d, *pre_parts[k])

        lanes = []
        for g in range(groups):
            for j in range(outer):
                lanes.append(hidden_keeps[g][:, j * count : (j + 1) * count])
                lanes.append(hidden_sends[g][:, j * count : (j + 1) * count])
        panel = jnp.concatenate(lanes, axis=1)
        grad_down, curv_down, partial = down_grads(core_line, panel, sign_down, *error_shards)
        grad_gate, curv_gate, grad_up, curv_up, packed = wide_grads(
            core_line, sign_gate, sign_up, partial, cots, token_pieces
        )
        packed = total_over_all(packed, (("row", n_row), ("col", n_col)))
        entries = 3.0 * feats * n_row * width * n_col
        scales = 1.0 / jnp.sqrt(packed[0, :2] / entries + 1e-06)
        results = update(
            scales,
            (
                (grad_gate, curv_gate, first_gate, second_gate),
                (grad_up, curv_up, first_up, second_up),
                (grad_down, curv_down, first_down, second_down),
            ),
        )
        return tuple(v if i % 3 == 2 else v.T for i, v in enumerate(results))

    def gather_blocks(block):
        got = [block]
        for _ in range(1, outer):
            got.append(ring_up(got[-1], "row", n_row))
        return got

    def by_owner(got, chip):
        return [pick(got, (chip - j) % outer) for j in range(outer)]

    return body


def solution(mesh):
    wide = P("row", "col")
    tall = P("col", "row")
    inner = make_body(mesh.shape["row"], mesh.shape["col"])

    return jax.shard_map(
        inner,
        mesh=mesh,
        in_specs=(tall, tall, wide, wide, tall, wide, wide, tall, wide, wide, tall, wide, wide, tall),
        out_specs=(wide, wide, tall, wide, wide, tall, wide, wide, tall),
        check_vma=False,
    )
```

```python
import jax
import jax.numpy as jnp
from jax import lax
from jax.experimental import pallas as pl
from jax.experimental.pallas import tpu as pltpu
from jax.sharding import PartitionSpec as P


STEP = 10
BF = jnp.bfloat16
F32 = jnp.float32


def dot(left, right, inner):
    return lax.dot_general(left, right, (((inner[0],), (inner[1],)), ((), ())), preferred_element_type=F32)


def pick(blocks, index):
    chosen = blocks[0]
    for at in range(1, len(blocks)):
        chosen = jnp.where(index == at, blocks[at], chosen)
    return chosen


def pair_swap(value, axis, size):
    return lax.ppermute(value, axis, [(i, i ^ 1) for i in range(size)])


def ring_up(value, axis, size):
    return lax.ppermute(value, axis, [(i, (i + 2) % size) for i in range(size)])


def ring_up_apart(value, n_row, n_col):
    perm = []
    for r in range(n_row):
        for c in range(n_col):
            perm.append((r * n_col + c, r * n_col + ((c + 2) % n_col ^ (r % 2))))
    return lax.ppermute(value, ("row", "col"), perm)


def total_over_all(value, sizes):
    for axis, size in sizes:
        step = 1
        while step < size:
            if size % (2 * step) == 0:
                value = value + lax.ppermute(value, axis, [(i, i ^ step) for i in range(size)])
                step *= 2
            else:
                raise ValueError("axis size")
    return value


def sign_kernel(gate_ref, up_ref, probe_gate_ref, probe_up_ref, probe_down_ref, wide_ref, down_ref):
    width = gate_ref.shape[0]
    wide_ref[:width] = gate_ref[...]
    wide_ref[width : 2 * width] = up_ref[...]
    for at, probe in ((2, probe_gate_ref), (3, probe_up_ref)):
        wide_ref[at * width : (at + 1) * width] = (2 * probe[...] - 1).astype(F32).astype(BF)
    down_ref[...] = (2 * probe_down_ref[...] - 1).astype(F32).astype(BF)


def side(feats, best=512):
    while feats % best:
        best //= 2
    return best


def cols_tile(rows, tile):
    return pl.BlockSpec((rows, tile), lambda i: (0, i))


def fixed(shape):
    return pl.BlockSpec(shape, lambda i: (0, 0))


def signs(*arrays):
    width, feats = arrays[0].shape
    tile = side(feats, 256)
    return pl.pallas_call(
        sign_kernel,
        grid=(feats // tile,),
        in_specs=[cols_tile(width, tile)] * 5,
        out_specs=[cols_tile(4 * width, tile), cols_tile(width, tile)],
        out_shape=[jax.ShapeDtypeStruct((n * width, feats), BF) for n in (4, 1)],
        name="signs",
    )(*arrays)


def same_block():
    down = lax.broadcasted_iota(jnp.int32, (256, 256), 0) >> 2
    across = lax.broadcasted_iota(jnp.int32, (256, 256), 1) >> 2
    return jnp.where(down == across, 1.0, 0.0).astype(BF)


def finish_weight(grad, hess, sign, grad_ref, curv_ref, grad_sum, curv_sum):
    height, breadth = hess.shape
    grad_ref[...] = grad.astype(grad_ref.dtype)
    grad_sum[...] += jnp.sum(grad * grad, axis=0, keepdims=True)
    same = same_block()
    size = jnp.abs(sign.astype(F32) * hess).astype(BF)
    for left in range(0, breadth, 256):
        wide = min(256, breadth - left)
        lanes = slice(left, left + wide)
        total = curv_sum[:, lanes]
        for top in range(0, height, 256):
            tall = min(256, height - top)
            sums = jnp.dot(
                same[:tall, :tall], size[top : top + tall, lanes], preferred_element_type=F32
            )
            means = jnp.dot(
                (sums * 0.0625).astype(BF), same[:wide, :wide], preferred_element_type=F32
            )
            curv_ref[top : top + tall, lanes] = means.astype(curv_ref.dtype)
            total = total + jnp.sum(means * means, axis=0, keepdims=True)
        curv_sum[:, lanes] = total


def pack_sums(grad_sum, curv_sum):
    lane = lax.broadcasted_iota(jnp.int32, (8, 128), 1)
    first = jnp.where(lane == 0, jnp.sum(grad_sum[...]), 0.0)
    return jnp.where(lane == 1, jnp.sum(curv_sum[...]), first)


def stacked(refs):
    return jnp.concatenate([r[...] for r in refs], axis=0)


def down_kernel(pieces, *refs):
    panel_ref, sign_ref = refs[:2]
    err_refs = refs[2 : 2 + pieces]
    dot_refs = refs[2 + pieces : 2 + 2 * pieces]
    grad_ref, curv_ref, pack_ref, grad_sum, curv_sum = refs[2 + 2 * pieces :]

    @pl.when(pl.program_id(0) == 0)
    def _():
        grad_sum[...] = jnp.zeros_like(grad_sum)
        curv_sum[...] = jnp.zeros_like(curv_sum)

    width = sign_ref.shape[0]
    err = stacked(err_refs)
    err_dot = stacked(dot_refs)
    plain = panel_ref[:width, :]
    grad = jnp.dot(plain, err, preferred_element_type=F32)
    hess = jnp.dot(panel_ref[width:, :], err, preferred_element_type=F32)
    hess = hess + jnp.dot(plain, err_dot, preferred_element_type=F32)
    finish_weight(grad, hess, sign_ref[...], grad_ref, curv_ref, grad_sum, curv_sum)

    @pl.when(pl.program_id(0) == pl.num_programs(0) - 1)
    def _():
        pack_ref[...] = pack_sums(grad_sum, curv_sum)


def down_grads(panel, sign, errs, dots):
    width, feats = sign.shape
    tile = side(feats)
    each = [cols_tile(errs[0].shape[0], tile)] * len(errs)
    return pl.pallas_call(
        lambda *refs: down_kernel(len(errs), *refs),
        grid=(feats // tile,),
        in_specs=[
            fixed(panel.shape), cols_tile(width, tile), *each, *each
        ],
        out_specs=[cols_tile(width, tile), cols_tile(width, tile), fixed((8, 128))],
        out_shape=[
            jax.ShapeDtypeStruct((width, feats), BF),
            jax.ShapeDtypeStruct((width, feats), BF),
            jax.ShapeDtypeStruct((8, 128), F32),
        ],
        scratch_shapes=[pltpu.VMEM((1, tile), F32), pltpu.VMEM((1, tile), F32)],
        compiler_params=pltpu.CompilerParams(dimension_semantics=("arbitrary",)),
        cost_estimate=pl.CostEstimate(
            flops=6 * width * feats * panel.shape[1], transcendentals=0, bytes_accessed=12 * width * feats
        ),
        name="down_grads",
    )(panel, sign, *errs, *dots)


def cotangents(d_refs, by_refs, cot_ref):
    width = d_refs[0].shape[0] // 2
    chunk = 16 if width % 16 == 0 else width

    def step(i, carry):
        def at(ref, n):
            return ref[pl.ds(pl.multiple_of(n * width + i * chunk, chunk), chunk), :].astype(F32)

        for shard, (d_ref, by_ref) in enumerate(zip(d_refs, by_refs)):
            count = d_ref.shape[1]
            d_hidden, d_hidden_dot = at(d_ref, 0), at(d_ref, 1)
            for_gate, for_up = at(by_ref, 0), at(by_ref, 1)
            for n, value in enumerate(
                (
                    d_hidden * for_gate,
                    d_hidden * for_up,
                    d_hidden_dot * for_gate + d_hidden * at(by_ref, 2),
                    d_hidden_dot * for_up + d_hidden * at(by_ref, 3),
                )
            ):
                rows = pl.ds(pl.multiple_of(n * width + i * chunk, chunk), chunk)
                cot_ref[rows, shard * count : (shard + 1) * count] = value.astype(BF)
        return carry

    lax.fori_loop(0, width // chunk, step, 0)


def wide_kernel(shards, *refs):
    sign_gate_ref, sign_up_ref, before_ref = refs[:3]
    token_refs, d_refs, by_refs = (refs[3 + n * shards : 3 + (n + 1) * shards] for n in range(3))
    grad_gate_ref, curv_gate_ref, grad_up_ref, curv_up_ref, pack_ref, grad_sum, curv_sum, cot_ref = refs[
        3 + 3 * shards :
    ]

    @pl.when(pl.program_id(0) == 0)
    def _():
        grad_sum[...] = jnp.zeros_like(grad_sum)
        curv_sum[...] = jnp.zeros_like(curv_sum)
        cotangents(d_refs, by_refs, cot_ref)

    width = sign_gate_ref.shape[0]
    tokens = stacked(token_refs)

    def product(at):
        return jnp.dot(cot_ref[at * width : (at + 1) * width, :], tokens, preferred_element_type=F32)

    finish_weight(
        product(0), product(2), sign_gate_ref[...], grad_gate_ref, curv_gate_ref, grad_sum, curv_sum
    )
    finish_weight(product(1), product(3), sign_up_ref[...], grad_up_ref, curv_up_ref, grad_sum, curv_sum)

    @pl.when(pl.program_id(0) == pl.num_programs(0) - 1)
    def _():
        pack_ref[...] = before_ref[...] + pack_sums(grad_sum, curv_sum)


def wide_grads(weights, before, tokens, ds, bys):
    feats = weights.shape[1]
    width = weights.shape[0] // 4
    tile = side(feats, 256)
    out = cols_tile(width, tile)
    count = tokens[0].shape[0] * len(tokens)
    return pl.pallas_call(
        lambda *refs: wide_kernel(len(tokens), *refs),
        grid=(feats // tile,),
        in_specs=[
            pl.BlockSpec((width, tile), lambda i: (2, i)),
            pl.BlockSpec((width, tile), lambda i: (3, i)),
            fixed((8, 128)),
            *[cols_tile(t.shape[0], tile) for t in tokens],
            *[fixed(d.shape) for d in ds],
            *[fixed(b.shape) for b in bys],
        ],
        out_specs=[out, out, out, out, fixed((8, 128))],
        out_shape=[jax.ShapeDtypeStruct((width, feats), BF)] * 4 + [jax.ShapeDtypeStruct((8, 128), F32)],
        scratch_shapes=[
            pltpu.VMEM((1, tile), F32), pltpu.VMEM((1, tile), F32), pltpu.VMEM((4 * width, count), BF)
        ],
        compiler_params=pltpu.CompilerParams(dimension_semantics=("arbitrary",)),
        cost_estimate=pl.CostEstimate(
            flops=8 * width * feats * count, transcendentals=0, bytes_accessed=20 * width * feats
        ),
        name="wide_grads",
    )(weights, weights, before, *tokens, *ds, *bys)


def update_kernel(scale_ref, *refs):
    fix_first = 1.0 - 0.9**STEP
    fix_second = 1.0 - 0.95**STEP
    by_grad = scale_ref[0]
    by_curv = scale_ref[1]
    for at in range(3):
        grad, curv, first, second = (refs[4 * at + n][...].astype(F32) for n in range(4))
        first_ref, second_ref, update_ref = (refs[12 + 3 * n + at] for n in range(3))
        new_first = 0.9 * first + 0.1 * (grad * by_grad)
        scaled = curv * by_curv
        new_second = 0.95 * second + 0.05 * (scaled * scaled)
        first_ref[...] = new_first
        second_ref[...] = new_second
        update_ref[...] = new_first * (1.0 / fix_first) / (jnp.sqrt(new_second * (1.0 / fix_second)) + 1e-08)


def update(scales, weights):
    width, feats = weights[0][0].shape
    tall = cols_tile(width, 128)
    shapes = [jax.ShapeDtypeStruct(w[0].shape, F32) for w in weights]
    return pl.pallas_call(
        update_kernel,
        grid=(feats // 128,),
        in_specs=[pl.BlockSpec(memory_space=pltpu.SMEM)] + [tall] * 12,
        out_specs=[tall] * 9,
        out_shape=shapes * 3,
        name="update",
    )(scales, *weights[0], *weights[1], *weights[2])


def activation(pre):
    sig = jax.nn.sigmoid(pre)
    act = pre * sig
    slope = sig * (1.0 + pre * (1.0 - sig))
    bend = sig * (1.0 - sig) * (2.0 + pre * (1.0 - 2.0 * sig))
    return (act, slope, bend)


def make_body(n_row, n_col):
    outer = n_row // 2
    rings = n_col // 2
    groups = rings // outer
    if n_row % 2 or n_col % 2 or rings % outer:
        raise ValueError("mesh")

    def pass_on(k, current):
        other = pair_swap(current, "col", n_col)
        if k > 0:
            following = ring_up(current, "col", n_col) if k < rings - 1 else None
            return following, current, other
        following = ring_up_apart(current, n_row, n_col) if rings > 1 else None
        core = lax.axis_index("row") % 2
        keep = jnp.where(core == 0, current, other)
        return following, keep, jnp.where(core == 0, other, current)

    def body(
        tokens, target, gate_weight, up_weight, down_weight, probe_gate, probe_up, probe_down,
        first_gate, first_up, first_down, second_gate, second_up, second_down,
    ):
        row = lax.axis_index("row")
        core = row % 2
        chip = row // 2
        gate_weight, up_weight, probe_gate, probe_up, first_gate, first_up, second_gate, second_up = (
            v.T
            for v in (
                gate_weight, up_weight, probe_gate, probe_up, first_gate, first_up, second_gate, second_up
            )
        )
        width, feats = gate_weight.shape
        count = tokens.shape[0]
        wide_weights, sign_down = signs(gate_weight, up_weight, probe_gate, probe_up, probe_down)

        token_shards = []
        pre_keeps = []
        current = tokens
        for k in range(rings):
            current, keep, send = pass_on(k, current)
            token_shards += [keep, send]
            both = dot(wide_weights, jnp.concatenate([send, keep], axis=0), (1, 1))
            sent = both[:, :count].astype(BF)
            pre_keeps.append(both[:, count:] + pair_swap(sent, "row", n_row).astype(F32))

        hidden_keeps = []
        hidden_sends = []
        owned = []
        for g in range(groups):
            mine = pre_keeps[g * outer : (g + 1) * outer]
            current = pick(mine, (chip - 1) % outer)
            for s in range(1, outer):
                got = ring_up(current.astype(BF), "row", n_row)
                current = got.astype(F32) + pick(mine, (chip - s - 1) % outer)
            pre_gate = current[:width]
            pre_up = current[width : 2 * width]
            dot_gate = current[2 * width : 3 * width]
            dot_up = current[3 * width :]
            act, slope, bend = activation(pre_gate)
            owned.append(
                jnp.concatenate(
                    [
                        (pre_up * slope).astype(BF),
                        act.astype(BF),
                        (dot_up * slope + pre_up * bend * dot_gate).astype(BF),
                        (slope * dot_gate).astype(BF),
                    ],
                    axis=0,
                )
            )
            hidden = (act * pre_up).astype(BF)
            hidden_dot = (slope * dot_gate * pre_up + act * dot_up).astype(BF)
            keeps = by_owner(gather_blocks(jnp.concatenate([hidden, hidden_dot], axis=0)), chip)
            both = jnp.concatenate(keeps, axis=1)
            sends = pair_swap(both, "row", n_row)
            hidden_keeps.append(both)
            hidden_sends.append(sends)

        near = ([], [])
        far = ([], [])
        for g in range(groups):
            sides = []
            for panel in (hidden_keeps[g], hidden_sends[g]):
                value = dot(panel[:width], down_weight, (0, 0))
                along = dot(panel[width:], down_weight, (0, 0)) + dot(panel[:width], sign_down, (0, 0))
                sides.append((value, along))
            for j in range(outer):
                for part in range(2):
                    own = sides[0][part][j * count : (j + 1) * count]
                    alien = sides[1][part][j * count : (j + 1) * count]
                    near[part].append(jnp.where(core == 0, own, alien))
                    far[part].append(jnp.where(core == 0, alien, own).astype(BF))
        order = [*range(1, rings), 0]
        reduced = {}
        for k in order:
            for part in range(2):
                reduced[k, part] = near[part][k] + pair_swap(far[part][k], "col", n_col).astype(F32)
        outputs = [reduced[order[0], part] for part in range(2)]
        for k in order[1:]:
            for part in range(2):
                moved = ring_up(outputs[part].astype(BF), "col", n_col)
                outputs[part] = moved.astype(F32) + reduced[k, part]
        errors = [(outputs[0] - target.astype(F32)).astype(BF), outputs[1].astype(BF)]

        error_shards = ([], [])
        ds = []
        bys = []
        for k in range(rings):
            if k == min(1, rings - 1):
                for g in range(groups):
                    got = gather_blocks(owned[g])
                    errors[0], *got = lax.optimization_barrier((errors[0], *got))
                    for keeps in by_owner(got, chip):
                        bys += [keeps, pair_swap(keeps, "row", n_row)]
            for part in range(2):
                errors[part], keep, send = pass_on(k, errors[part])
                error_shards[part].extend([keep, send])

            def term(at):
                err, err_dot = error_shards[0][2 * k + at], error_shards[1][2 * k + at]
                plain = dot(down_weight, err, (1, 1))
                along = dot(down_weight, err_dot, (1, 1)) + dot(sign_down, err, (1, 1))
                return plain, along

            sent = jnp.concatenate([v.astype(BF) for v in term(1)], axis=0)
            kept = jnp.concatenate(term(0), axis=0)
            total = kept + pair_swap(sent, "row", n_row).astype(F32)
            moving = total.astype(BF)
            for _ in range(1, outer):
                moving = ring_up(moving, "row", n_row)
                total = total + moving.astype(F32)
            keep_d = total.astype(BF)
            ds += [keep_d, pair_swap(keep_d, "row", n_row)]

        lanes = []
        for g in range(groups):
            for j in range(outer):
                lanes.append(hidden_keeps[g][:, j * count : (j + 1) * count])
                lanes.append(hidden_sends[g][:, j * count : (j + 1) * count])
        panel = jnp.concatenate(lanes, axis=1)
        grad_down, curv_down, partial = down_grads(panel, sign_down, *error_shards)
        grad_gate, curv_gate, grad_up, curv_up, packed = wide_grads(
            wide_weights, partial, token_shards, ds, bys
        )
        packed = total_over_all(packed, (("row", n_row), ("col", n_col)))
        entries = 3.0 * feats * n_row * width * n_col
        scales = 1.0 / jnp.sqrt(packed[0, :2] / entries + 1e-06)
        results = update(
            scales,
            (
                (grad_gate, curv_gate, first_gate, second_gate),
                (grad_up, curv_up, first_up, second_up),
                (grad_down, curv_down, first_down, second_down),
            ),
        )
        return tuple(v if i % 3 == 2 else v.T for i, v in enumerate(results))

    def gather_blocks(block):
        got = [block]
        for _ in range(1, outer):
            got.append(ring_up(got[-1], "row", n_row))
        return got

    def by_owner(got, chip):
        return [pick(got, (chip - j) % outer) for j in range(outer)]

    return body


def solution(mesh):
    wide = P("row", "col")
    tall = P("col", "row")
    inner = make_body(mesh.shape["row"], mesh.shape["col"])

    return jax.shard_map(
        inner,
        mesh=mesh,
        in_specs=(tall, tall, wide, wide, tall, wide, wide, tall, wide, wide, tall, wide, wide, tall),
        out_specs=(wide, wide, tall, wide, wide, tall, wide, wide, tall),
        check_vma=False,
    )
```
